32 devices in a mesh: col: 4 (over z), row: 8 (over y, x, core).
Axes of the slice: x: 2, y: 2, z: 4, core: 2. Of those that a mesh axis runs over, the one named last changes fastest.
Arguments:
- x_in: bfloat16 [2, 128, 1024, 256], P(None, 'row', 'col')
- a_pre: bfloat16 [2, 128, 1024, 256], P(None, 'row', 'col')
- g_out: bfloat16 [2, 128, 1024, 256], P(None, 'row', 'col')
- w_one: bfloat16 [3, 3, 256, 256], replicated
- w_two: bfloat16 [3, 3, 256, 256], replicated
Outputs:
- output 1: bfloat16 [2, 128, 1024, 256], P(None, 'row', 'col')
- output 2: float32 [3, 3, 256, 256], replicated
- output 3: float32 [3, 3, 256, 256], replicated
All inputs are finite; a program needn't handle non-finite values.
Results may differ from the reference program's by a relative error of at most 0.001.
Values are sent between devices in bfloat16 or wider.
A program may use at most 1 GiB of HBM per device.

```python
import jax
import jax.numpy as jnp
from jax import lax

IMAGES = 2
CHANNELS = 256
TILE_ROWS = 16
TILE_COLS = 256
IMG_HEIGHT = 128
IMG_WIDTH = 1024

FRAME_PAD = ((0, 0), (1, 1), (1, 1), (0, 0))


def conv_same(image_in, kernel):
    return lax.conv_general_dilated(image_in, kernel, (1, 1), "SAME", dimension_numbers=("NHWC", "HWIO", "NHWC"))


def gelu_slope(pre_act):
    tanh_scale = 0.7978845608028654
    cube_coef = 0.044715
    tanh_val = jnp.tanh(tanh_scale * (pre_act + cube_coef * pre_act * pre_act * pre_act))
    return 0.5 * (1.0 + tanh_val) + 0.5 * pre_act * (1.0 - tanh_val * tanh_val) * tanh_scale * (1.0 + 3.0 * cube_coef * pre_act * pre_act)


def tap_grads(left_pad, right_img):
    row_count = right_img.shape[1]
    col_count = right_img.shape[2]
    return jnp.stack([jnp.stack([jnp.einsum("bhwi,bhwo->io", left_pad[:, tap_row:tap_row + row_count, tap_col:tap_col + col_count], right_img) for tap_col in range(3)]) for tap_row in range(3)])


def edge_weight(boost):
    row_pos = jnp.arange(IMG_HEIGHT) % TILE_ROWS
    col_pos = jnp.arange(IMG_WIDTH) % TILE_COLS
    row_edge = (row_pos == 0) | (row_pos == TILE_ROWS - 1)
    col_edge = (col_pos == 0) | (col_pos == TILE_COLS - 1)
    on_edge = (row_edge[:, None] | col_edge[None, :]).astype(jnp.float32)
    return (1.0 + boost * on_edge)[None, :, :, None]


def setup_inputs(seed: int = 0) -> dict:
    key = jax.random.key(seed)
    key_x, key_a, key_g, key_one, key_two = jax.random.split(key, 5)
    img_shape = (IMAGES, IMG_HEIGHT, IMG_WIDTH, CHANNELS)
    fan_scale = (9 * CHANNELS) ** -0.5
    x_in = jax.random.normal(key_x, img_shape, jnp.float32).astype(jnp.bfloat16)
    a_pre = jax.random.normal(key_a, img_shape, jnp.float32).astype(jnp.bfloat16)
    g_out = (jax.random.normal(key_g, img_shape, jnp.float32) * edge_weight(2.0)).astype(jnp.bfloat16)
    w_one = (jax.random.normal(key_one, (3, 3, CHANNELS, CHANNELS), jnp.float32) * fan_scale).astype(jnp.bfloat16)
    w_two = (jax.random.normal(key_two, (3, 3, CHANNELS, CHANNELS), jnp.float32) * fan_scale).astype(jnp.bfloat16)
    return {"x_in": x_in, "a_pre": a_pre, "g_out": g_out, "w_one": w_one, "w_two": w_two}


def reference(x_in, a_pre, g_out, w_one, w_two):
    w_one_f = w_one.astype(jnp.float32)
    w_two_f = w_two.astype(jnp.float32)

    def conv_first(image_in):
        return conv_same(image_in, w_one_f)

    def conv_second(image_in):
        return conv_same(image_in, w_two_f)

    def one_image(packed):
        x_img, a_img, g_img = packed
        x_val = x_img[None].astype(jnp.float32)
        a_val = a_img[None].astype(jnp.float32)
        g_val = g_img[None].astype(jnp.float32)
        z_act = jax.nn.gelu(a_val, approximate=True).astype(jnp.bfloat16).astype(jnp.float32)
        d_z = jax.vjp(conv_second, z_act)[1](g_val)[0]
        d_w2 = tap_grads(jnp.pad(z_act, FRAME_PAD), g_val)
        d_a = (d_z * gelu_slope(a_val)).astype(jnp.bfloat16).astype(jnp.float32)
        conv_grad = jax.vjp(conv_first, x_val)[1](d_a)[0]
        d_w1 = tap_grads(jnp.pad(x_val, FRAME_PAD), d_a)
        d_x = (conv_grad + g_val).astype(jnp.bfloat16)
        return d_x[0], d_w1, d_w2

    d_x, w1_parts, w2_parts = lax.map(one_image, (x_in, a_pre, g_out))
    return d_x, jnp.sum(w1_parts, axis=0), jnp.sum(w2_parts, axis=0)
```

```python
import functools

import jax
import jax.numpy as jnp
from jax import lax
from jax.experimental import pallas as pl
from jax.experimental.pallas import tpu as pltpu
from jax.sharding import PartitionSpec as P

MESH = pl.DeviceIdType.MESH
F32 = jnp.float32
BF16 = jnp.bfloat16

IMGS, ROWS, COLS, CH = 2, 16, 256, 256
STRIP = 8
BLK = 4
HALF = BLK // 2
NBLK = IMGS * ROWS // BLK
CHUNK = 16
NCHUNK = IMGS * ROWS // CHUNK
DIRS = ((1, 0), (-1, 0), (0, 1), (0, -1), (1, 1), (1, -1), (-1, 1), (-1, -1))
CORE, XBIT, YBIT, ZNEAR, ZFAR = ("row", 1), ("row", 2), ("row", 4), ("col", 1), ("col", 2)
ORDERS = ((CORE, XBIT, YBIT, ZNEAR, ZFAR), (CORE, YBIT, ZNEAR, ZFAR, XBIT), (CORE, ZNEAR, ZFAR, XBIT, YBIT))
NSTEP = 5
PIX = 128
SUB = 32
RECV_AT = (0, 128, 192, 224, 240)

EARLY = (1, 3, 4, 5, 7, 8, 9, 10, 12, 13)
LATE = (1, 2, 3, 4, 5, 6, 7, 8, 9, 10)


def gelu_tanh(a_val):
    scale = 0.7978845608028654
    square = (0.044715 * a_val) * a_val
    return jnp.tanh(scale * (a_val + square * a_val)), square


def gelu(a_val):
    tanh_val, _ = gelu_tanh(a_val)
    half = 0.5 * a_val
    return half + half * tanh_val


def gelu_slope(a_val):
    scale = 0.7978845608028654
    tanh_val, square = gelu_tanh(a_val)
    return (0.5 + 0.5 * tanh_val) + ((0.5 * a_val) * (1.0 - tanh_val * tanh_val)) * (scale * (1.0 + 3.0 * square))


def kernel(x_hbm, a_hbm, g_hbm, w1_hbm, w2_hbm, dx_hbm, dw1_hbm, dw2_hbm,
           gc, gs, dc, ds, abuf, zt, xt, w1t, w2t, wraw, acc, rbuf, res, s0, s1, ghl, ghr, dhl, dhr,
           load_sem, x_sem, out_sem, w_sem, gs_sem, gr_sem, ds_sem, dr_sem, as_sem, ar_sem):
    row = lax.axis_index("row")
    col = lax.axis_index("col")
    nrow, ncol = 8, 4

    def bit_of(axis, bit):
        where = row if axis == "row" else col
        return lax.rem(lax.div(where, bit), 2)

    def partner(axis, bit):
        flip = bit * (1 - 2 * bit_of(axis, bit))
        return {"row": row + flip, "col": col} if axis == "row" else {"row": row, "col": col + flip}

    def inside(d_row, d_col):
        ok = None
        for where, step, count in ((row, d_row, nrow), (col, d_col, ncol)):
            if step:
                cond = where < count - 1 if step > 0 else where > 0
                ok = cond if ok is None else jnp.logical_and(ok, cond)
        return ok

    barrier = pltpu.get_barrier_semaphore()
    for d_row, d_col in DIRS:
        @pl.when(inside(d_row, d_col))
        def _(d_row=d_row, d_col=d_col):
            pl.semaphore_signal(barrier, inc=1, device_id={"row": row + d_row, "col": col + d_col}, device_id_type=MESH)
    for axis, bit in ORDERS[0]:
        pl.semaphore_signal(barrier, inc=1, device_id=partner(axis, bit), device_id_type=MESH)

    g_loads = [pltpu.make_async_copy(g_hbm.at[i], gc.at[i, pl.ds(1, ROWS)], load_sem.at[i]) for i in range(IMGS)]
    a_loads = [pltpu.make_async_copy(a_hbm.at[i], abuf.at[i], load_sem.at[IMGS + i]) for i in range(IMGS)]
    w_load2 = pltpu.make_async_copy(w2_hbm, wraw, w_sem.at[0])
    w_load1 = pltpu.make_async_copy(w1_hbm, wraw, w_sem.at[1])
    w_load2.start()
    for load in g_loads + a_loads:
        load.start()

    x_loads = [pltpu.make_async_copy(x_hbm.at[i], dc.at[i, pl.ds(1, ROWS)], x_sem.at[i]) for i in range(IMGS)]

    def near(where, count):
        return 3 - jnp.where(where == 0, 1, 0) - jnp.where(where == count - 1, 1, 0)

    pl.semaphore_wait(barrier, NSTEP + near(row, nrow) * near(col, ncol) - 1)

    def halo_copy(src, row0, mid, left, right, send_sem, recv_sem, i, n):
        d_row, d_col = DIRS[n]
        s_row = pl.ds(row0, ROWS) if d_row == 0 else (row0 + ROWS - 1 if d_row > 0 else row0)
        t_row = pl.ds(1, ROWS) if d_row == 0 else (0 if d_row > 0 else ROWS + 1)
        if d_col == 0:
            s_ref, t_ref = src.at[i, s_row], mid.at[i, t_row]
        else:
            s_col = pl.ds(COLS - STRIP, STRIP) if d_col > 0 else pl.ds(0, STRIP)
            s_ref, t_ref = src.at[i, s_row, s_col], (left if d_col > 0 else right).at[i, t_row]
        return pltpu.make_async_remote_copy(src_ref=s_ref, dst_ref=t_ref, send_sem=send_sem.at[i, n], recv_sem=recv_sem.at[i, n],
                                            device_id={"row": row + d_row, "col": col + d_col}, device_id_type=MESH)

    def halo_start(*args):
        for n, (d_row, d_col) in enumerate(DIRS):
            @pl.when(inside(d_row, d_col))
            def _(n=n):
                halo_copy(*args, n).start()

    def halo_wait(*args):
        for n, (d_row, d_col) in enumerate(DIRS):
            @pl.when(inside(d_row, d_col))
            def _(n=n):
                halo_copy(*args, n).wait_send()

            @pl.when(inside(-d_row, -d_col))
            def _(n=n):
                halo_copy(*args, n).wait_recv()

    def halo_zero(mid, left, right):
        @pl.when(row == 0)
        def _():
            for i in range(IMGS):
                mid[i, 0] = jnp.zeros((COLS, CH), BF16)
                left[i, 0] = jnp.zeros((STRIP, CH), BF16)
                right[i, 0] = jnp.zeros((STRIP, CH), BF16)

        @pl.when(row == nrow - 1)
        def _():
            for i in range(IMGS):
                mid[i, ROWS + 1] = jnp.zeros((COLS, CH), BF16)
                left[i, ROWS + 1] = jnp.zeros((STRIP, CH), BF16)
                right[i, ROWS + 1] = jnp.zeros((STRIP, CH), BF16)

        for side, edge in ((left, 0), (right, ncol - 1)):
            @pl.when(col == edge)
            def _(side=side):
                @pl.loop(0, ROWS + 2)
                def _(r):
                    for i in range(IMGS):
                        side[i, r] = jnp.zeros((STRIP, CH), BF16)

    def store_sides(mid, side, i, r):
        for lane in range(0, CH, 128):
            val = mid[i, r, :, lane:lane + 128].astype(F32)
            side[i, r, :, lane:lane + 128] = pltpu.roll(val, COLS - 1, axis=0).astype(BF16)
            side[i, r, :, CH + lane:CH + lane + 128] = pltpu.roll(val, 1, axis=0).astype(BF16)

    def fix_edges(mid, side, left, right, i):
        for r in (0, ROWS + 1):
            store_sides(mid, side, i, r)
        at = lax.broadcasted_iota(jnp.int32, (STRIP, CH), 0)

        @pl.loop(0, ROWS + 2)
        def _(r):
            here = side[i, r, 0:STRIP, CH:2 * CH].astype(F32)
            other = pltpu.roll(left[i, r].astype(F32), 1, axis=0)
            side[i, r, 0:STRIP, CH:2 * CH] = jnp.where(at == 0, other, here).astype(BF16)
            here = side[i, r, COLS - STRIP:COLS, 0:CH].astype(F32)
            other = pltpu.roll(right[i, r].astype(F32), STRIP - 1, axis=0)
            side[i, r, COLS - STRIP:COLS, 0:CH] = jnp.where(at == STRIP - 1, other, here).astype(BF16)

    g_halo = (g_hbm, 0, gc, ghl, ghr, gs_sem, gr_sem)
    d_halo = (dc, 1, dc, dhl, dhr, ds_sem, dr_sem)
    for i in range(IMGS):
        halo_start(*g_halo, i)
    halo_zero(gc, ghl, ghr)
    halo_zero(dc, dhl, dhr)

    w_load2.wait()

    def slot_of(k):
        return k - lax.rem(k, 3) + lax.rem(2 * lax.rem(k, 3), 3)

    @pl.loop(0, 9)
    def _(k):
        w2t[slot_of(k)] = wraw[k].T

    w_load1.start()
    for load in x_loads:
        load.start()
    for i in range(IMGS):
        g_loads[i].wait()

        @pl.loop(0, ROWS)
        def _(r, i=i):
            store_sides(gc, gs, i, r + 1)

    def act_row(i, r):
        for j in range(0, COLS, PIX):
            z_val = gelu(abuf[i, r, j:j + PIX].astype(F32))
            zt[:, pl.ds(pl.multiple_of((i * ROWS + r) * COLS + j, PIX), PIX)] = z_val.astype(BF16).T

    for i in range(IMGS):
        a_loads[i].wait()

        @pl.loop(0, ROWS)
        def _(r, i=i):
            act_row(i, r)

    def place(blk):
        return lax.div(blk, ROWS // BLK), lax.rem(blk, ROWS // BLK) * BLK

    def conv(mid, side, weights, blk):
        i, r0 = place(blk)
        for half, out in ((0, s0), (1, s1)):
            total = None
            for a in range(3):
                rows = pl.ds(r0 + half * HALF + 2 - a, HALF)
                part = jnp.dot(side[i, rows].reshape(HALF * COLS, 2 * CH), weights[3 * a:3 * a + 2].reshape(2 * CH, CH),
                               preferred_element_type=F32)
                part = part + jnp.dot(mid[i, rows].reshape(HALF * COLS, CH), weights[3 * a + 2], preferred_element_type=F32)
                total = part if total is None else total + part
            out[...] = total

    def held_part(k, j, size=PIX):
        at = (k % HALF) * COLS + j
        return (s0 if k < HALF else s1)[at:at + size]

    def grad_rows(blk):
        i, r0 = place(blk)
        for k in range(BLK):
            for j in range(0, COLS, SUB):
                slope = gelu_slope(abuf[i, r0 + k, j:j + SUB].astype(F32))
                dc[i, r0 + k + 1, j:j + SUB] = (held_part(k, j, SUB) * slope).astype(BF16)

    def shift_block(blk):
        i, r0 = place(blk)
        for k in range(BLK):
            store_sides(dc, ds, i, r0 + k + 1)

    def start_at(c, s):
        at = 0
        for j in range(s):
            at = at + bit_of(*ORDERS[c][j]) * (128 >> j)
        return at

    def reduce_copy(p, c, s):
        idx, h = p * 3 + c, 128 >> s
        mine = bit_of(*ORDERS[c][s])
        src = acc.at[idx, pl.ds(pl.multiple_of(start_at(c, s) + (1 - mine) * h, 8), h)]
        return pltpu.make_async_remote_copy(src_ref=src, dst_ref=rbuf.at[idx, pl.ds(RECV_AT[s], h)],
                                            send_sem=as_sem.at[idx, s], recv_sem=ar_sem.at[idx, s],
                                            device_id=partner(*ORDERS[c][s]), device_id_type=MESH)

    def gather_copy(p, c, s):
        idx, h = p * 3 + c, 128 >> s
        part = res.at[idx, pl.ds(pl.multiple_of(start_at(c, s + 1), 8), h)]
        return pltpu.make_async_remote_copy(src_ref=part, dst_ref=part,
                                            send_sem=as_sem.at[idx, NSTEP + s], recv_sem=ar_sem.at[idx, NSTEP + s],
                                            device_id=partner(*ORDERS[c][s]), device_id_type=MESH)

    def out_copy(p, c):
        target = dw2_hbm if p < 3 else dw1_hbm
        idx = p * 3 + c
        return pltpu.make_async_copy(res.at[idx], target.at[lax.rem(idx, 9)], out_sem.at[NBLK + idx])

    def reduce_start(p):
        for c in range(3):
            reduce_copy(p, c, 0).start()

    def reduce_step(p, step):
        for c in range(3):
            idx = p * 3 + c
            if step < NSTEP:
                s, h = step, 128 >> step
                reduce_copy(p, c, s).wait()
                keep = pl.ds(pl.multiple_of(start_at(c, s + 1), 8), h)
                (acc if s < NSTEP - 1 else res)[idx, keep] = acc[idx, keep] + rbuf[idx, RECV_AT[s]:RECV_AT[s] + h]
                if s < NSTEP - 1:
                    reduce_copy(p, c, s + 1).start()
                else:
                    gather_copy(p, c, s).start()
            else:
                s = 2 * NSTEP - 1 - step
                gather_copy(p, c, s).wait()
                if s > 0:
                    gather_copy(p, c, s - 1).start()
                else:
                    out_copy(p, c).start()

    grad_ticks = ((0, 0), (0, 1), (1, 0), (1, 1), (2, 0), (2, 1))
    late_ticks = ((3, 0), (4, 0), (3, 1), (4, 1), (5, 0), (5, 1))
    late_first = 3 * NCHUNK + NBLK - 1
    dx_first = late_first + len(late_ticks)
    last_tick = dx_first + NBLK - 1
    ready = {p: n + 1 for n, (p, _) in enumerate(grad_ticks)}
    ready.update({p: late_first + n + 1 for n, (p, _) in enumerate(late_ticks)})
    table = {}
    for p in range(6):
        for step, delay in enumerate(EARLY if p < 3 else LATE):
            table.setdefault(ready[p] + delay - 1, []).append((p, step))

    def run_steps(at):
        for p, step in table.get(at, ()):
            reduce_step(p, step)

    def tick(now, lo, hi):
        for at in sorted(table):
            if lo <= at < hi:
                @pl.when(now == at)
                def _(at=at):
                    run_steps(at)

    def weight_grad(p, n, lhs, mid, side):
        a = p % 3
        left = lhs[:, n * CHUNK * COLS:(n + 1) * CHUNK * COLS]
        part = jnp.dot(left, side[n, 2 - a:2 - a + CHUNK].reshape(CHUNK * COLS, 2 * CH), preferred_element_type=F32)
        part_mid = jnp.dot(left, mid[n, 2 - a:2 - a + CHUNK].reshape(CHUNK * COLS, CH), preferred_element_type=F32)
        for c, val in enumerate((part[:, :CH], part_mid, part[:, CH:])):
            acc[p * 3 + c] = val if n == 0 else acc[p * 3 + c] + val

    def turn_x(a, n):
        for k in range(6):
            r = min(a * 6 + k, ROWS - 1)
            for j in range(0, COLS, PIX):
                at = (n * ROWS + r) * COLS + j
                xt[:, at:at + PIX] = dc[n, r + 1, j:j + PIX].T

    def turn_weights(now):
        for k in range(2 * now, min(2 * now + 2, 9)):
            w1t[slot_of(k)] = wraw[k].T

    for i in range(IMGS):
        halo_wait(*g_halo, i)
        fix_edges(gc, gs, ghl, ghr, i)
    for load in x_loads:
        load.wait()
    for now, (p, n) in enumerate(grad_ticks):
        turn_x(p, n)
        weight_grad(p, n, zt, gc, gs)
        if n == 1:
            reduce_start(p)
        run_steps(now)

    half_blocks = NBLK // IMGS
    dz_first = 3 * NCHUNK
    dz_last = dz_first + NBLK - 1
    conv(gc, gs, w2t, 0)

    def dz_step(n):
        shift_block(jnp.maximum(n - 1, 0))
        grad_rows(n)
        conv(gc, gs, w2t, n + 1)
        tick(dz_first + n, dz_first, dz_last)

    @pl.loop(0, half_blocks)
    def _(n):
        dz_step(n)

    halo_start(*d_halo, 0)

    @pl.loop(half_blocks, NBLK - 1)
    def _(n):
        dz_step(n)

    grad_rows(NBLK - 1)
    halo_start(*d_halo, 1)
    shift_block(NBLK - 2)
    shift_block(NBLK - 1)
    halo_wait(*d_halo, 0)
    fix_edges(dc, ds, dhl, dhr, 0)
    w_load1.wait()

    for now, (p, n) in enumerate(late_ticks):
        if (p, n) == (3, 1):
            halo_wait(*d_halo, 1)
            fix_edges(dc, ds, dhl, dhr, 1)
        turn_weights(now)
        weight_grad(p, n, xt, dc, ds)
        if n == 1:
            reduce_start(p)
        run_steps(late_first + now)

    def dx_out(blk):
        i, r0 = place(blk)
        return pltpu.make_async_copy(abuf.at[i, pl.ds(r0, BLK)], dx_hbm.at[i, pl.ds(r0, BLK)], out_sem.at[blk])

    def dx_rows(blk):
        i, r0 = place(blk)
        for k in range(BLK):
            for j in range(0, COLS, PIX):
                g_val = gc[i, r0 + k + 1, j:j + PIX].astype(F32)
                abuf[i, r0 + k, j:j + PIX] = (held_part(k, j) + g_val).astype(BF16)

    conv(dc, ds, w1t, 0)

    @pl.loop(0, NBLK - 1)
    def _(n):
        dx_rows(n)
        conv(dc, ds, w1t, n + 1)
        dx_out(n).start()
        tick(dx_first + n, dx_first, last_tick)

    dx_rows(NBLK - 1)
    dx_out(NBLK - 1).start()
    for at in sorted(table):
        if at >= last_tick:
            run_steps(at)
    for blk in range(NBLK):
        dx_out(blk).wait()
    for p in range(6):
        for c in range(3):
            out_copy(p, c).wait()


def solution(mesh):
    def local_step(x_tile, a_tile, g_tile, w_one, w_two):
        wide = (IMGS, ROWS + 2, COLS, 2 * CH)
        tall = (IMGS, ROWS + 2, COLS, CH)
        side = (IMGS, ROWS + 2, STRIP, CH)
        any_spec = pl.BlockSpec(memory_space=pl.ANY)
        d_x, d_w1, d_w2 = pl.pallas_call(
            kernel,
            out_shape=(jax.ShapeDtypeStruct(x_tile.shape, BF16),
                       jax.ShapeDtypeStruct((9, CH, CH), F32), jax.ShapeDtypeStruct((9, CH, CH), F32)),
            in_specs=[any_spec] * 5,
            out_specs=(any_spec,) * 3,
            scratch_shapes=[
                pltpu.VMEM(tall, BF16), pltpu.VMEM(wide, BF16), pltpu.VMEM(tall, BF16), pltpu.VMEM(wide, BF16),
                pltpu.VMEM((IMGS, ROWS, COLS, CH), BF16),
                pltpu.VMEM((CH, IMGS * ROWS * COLS), BF16), pltpu.VMEM((CH, IMGS * ROWS * COLS), BF16),
                pltpu.VMEM((9, CH, CH), BF16), pltpu.VMEM((9, CH, CH), BF16), pltpu.VMEM((9, CH, CH), BF16),
                pltpu.VMEM((18, CH, CH), F32), pltpu.VMEM((18, CH, CH), F32), pltpu.VMEM((18, CH, CH), F32),
                pltpu.VMEM((HALF * COLS, CH), F32), pltpu.VMEM((HALF * COLS, CH), F32),
                pltpu.VMEM(side, BF16), pltpu.VMEM(side, BF16), pltpu.VMEM(side, BF16), pltpu.VMEM(side, BF16),
                pltpu.SemaphoreType.DMA((4,)), pltpu.SemaphoreType.DMA((2,)), pltpu.SemaphoreType.DMA((NBLK + 18,)),
                pltpu.SemaphoreType.DMA((2,)),
                pltpu.SemaphoreType.DMA((2, 8)), pltpu.SemaphoreType.DMA((2, 8)), pltpu.SemaphoreType.DMA((2, 8)), pltpu.SemaphoreType.DMA((2, 8)),
                pltpu.SemaphoreType.DMA((18, 2 * NSTEP)), pltpu.SemaphoreType.DMA((18, 2 * NSTEP)),
            ],
            compiler_params=pltpu.CompilerParams(collective_id=0, has_side_effects=True, vmem_limit_bytes=67043328),
            name="conv_block_backward",
        )(x_tile, a_tile, g_tile, w_one.reshape(9, CH, CH), w_two.reshape(9, CH, CH))
        return d_x, d_w1.reshape(3, 3, CH, CH), d_w2.reshape(3, 3, CH, CH)

    tile_spec = P(None, "row", "col", None)
    return jax.shard_map(local_step, mesh=mesh, in_specs=(tile_spec, tile_spec, tile_spec, P(), P()), out_specs=(tile_spec, P(), P()), check_vma=False)
```

```python
import functools

import jax
import jax.numpy as jnp
from jax import lax
from jax.experimental import pallas as pl
from jax.experimental.pallas import tpu as pltpu
from jax.sharding import PartitionSpec as P

MESH = pl.DeviceIdType.MESH
F32 = jnp.float32
BF16 = jnp.bfloat16

IMGS, ROWS, COLS, CH = 2, 16, 256, 256
STRIP = 8
BLK = 4
HALF = BLK // 2
NBLK = IMGS * ROWS // BLK
CHUNK = 16
NCHUNK = IMGS * ROWS // CHUNK
DIRS = ((1, 0), (-1, 0), (0, 1), (0, -1), (1, 1), (1, -1), (-1, 1), (-1, -1))
CORE, XBIT, YBIT, ZNEAR, ZFAR = ("row", 1), ("row", 2), ("row", 4), ("col", 1), ("col", 2)
STAGES = (((CORE,), (XBIT,), (YBIT,), (ZNEAR, ZFAR)),
          ((CORE,), (YBIT,), (XBIT,), (ZNEAR, ZFAR)),
          ((CORE,), (ZNEAR,), (ZFAR,), (XBIT, YBIT)))
PEERS = ((CORE,), (XBIT,), (YBIT,), (ZNEAR,), (ZFAR,), (XBIT, YBIT), (ZNEAR, ZFAR))
MAXCOPY = 6
PIX = 128

EARLY = (1, 3, 5, 6, 8, 9, 11, 12)
LATE = (1, 2, 3, 4, 5, 6, 7, 8)


def gelu_tanh(a_val):
    scale = 0.7978845608028654
    square = (0.044715 * a_val) * a_val
    return jnp.tanh(scale * (a_val + square * a_val)), square


def gelu(a_val):
    tanh_val, _ = gelu_tanh(a_val)
    half = 0.5 * a_val
    return half + half * tanh_val


def gelu_slope(a_val):
    scale = 0.7978845608028654
    tanh_val, square = gelu_tanh(a_val)
    return (0.5 + 0.5 * tanh_val) + ((0.5 * a_val) * (1.0 - tanh_val * tanh_val)) * (scale * (1.0 + 3.0 * square))


def kernel(x_hbm, a_hbm, g_hbm, w1_hbm, w2_hbm, dx_hbm, dw1_hbm, dw2_hbm,
           gc, gs, dc, ds, abuf, zt, xt, w1t, w2t, wraw, lines, acc, rbuf, res, s0, s1, ghl, ghr, dhl, dhr,
           load_sem, x_sem, out_sem, w_sem, gs_sem, gr_sem, ds_sem, dr_sem, as_sem, ar_sem):
    row = lax.axis_index("row")
    col = lax.axis_index("col")
    nrow, ncol = 8, 4

    def bit_of(axis, bit):
        where = row if axis == "row" else col
        return lax.rem(lax.div(where, bit), 2)

    def flips(stage, mask):
        return [key for n, key in enumerate(stage) if (mask >> (len(stage) - 1 - n)) & 1]

    def partner(stage, mask):
        where = {"row": row, "col": col}
        for axis, bit in flips(stage, mask):
            where[axis] = where[axis] + bit * (1 - 2 * bit_of(axis, bit))
        return where

    def seat(stage, mask=0):
        flipped = flips(stage, mask)
        at = 0
        for key in stage:
            at = 2 * at + (1 - bit_of(*key) if key in flipped else bit_of(*key))
        return at

    def inside(d_row, d_col):
        ok = None
        for where, step, count in ((row, d_row, nrow), (col, d_col, ncol)):
            if step:
                cond = where < count - 1 if step > 0 else where > 0
                ok = cond if ok is None else jnp.logical_and(ok, cond)
        return ok

    barrier = pltpu.get_barrier_semaphore()
    for d_row, d_col in DIRS:
        @pl.when(inside(d_row, d_col))
        def _(d_row=d_row, d_col=d_col):
            pl.semaphore_signal(barrier, inc=1, device_id={"row": row + d_row, "col": col + d_col}, device_id_type=MESH)
    for stage in PEERS:
        pl.semaphore_signal(barrier, inc=1, device_id=partner(stage, 2 ** len(stage) - 1), device_id_type=MESH)

    g_loads = [pltpu.make_async_copy(g_hbm.at[i], gc.at[i, pl.ds(1, ROWS)], load_sem.at[i]) for i in range(IMGS)]
    a_loads = [pltpu.make_async_copy(a_hbm.at[i], abuf.at[i], load_sem.at[IMGS + i]) for i in range(IMGS)]
    w_load2 = pltpu.make_async_copy(w2_hbm, wraw, w_sem.at[0])
    w_load1 = pltpu.make_async_copy(w1_hbm, wraw, w_sem.at[1])
    w_load2.start()
    for load in g_loads + a_loads:
        load.start()

    x_loads = [pltpu.make_async_copy(x_hbm.at[i], dc.at[i, pl.ds(1, ROWS)], x_sem.at[i]) for i in range(IMGS)]

    def near(where, count):
        return 3 - jnp.where(where == 0, 1, 0) - jnp.where(where == count - 1, 1, 0)

    pl.semaphore_wait(barrier, len(PEERS) + near(row, nrow) * near(col, ncol) - 1)

    def halo_copy(src, row0, mid, left, right, send_sem, recv_sem, i, n):
        d_row, d_col = DIRS[n]
        s_row = pl.ds(row0, ROWS) if d_row == 0 else (row0 + ROWS - 1 if d_row > 0 else row0)
        t_row = pl.ds(1, ROWS) if d_row == 0 else (0 if d_row > 0 else ROWS + 1)
        if d_col == 0:
            s_ref, t_ref = src.at[i, s_row], mid.at[i, t_row]
        else:
            s_col = pl.ds(COLS - STRIP, STRIP) if d_col > 0 else pl.ds(0, STRIP)
            s_ref, t_ref = src.at[i, s_row, s_col], (left if d_col > 0 else right).at[i, t_row]
        return pltpu.make_async_remote_copy(src_ref=s_ref, dst_ref=t_ref, send_sem=send_sem.at[i, n], recv_sem=recv_sem.at[i, n],
                                            device_id={"row": row + d_row, "col": col + d_col}, device_id_type=MESH)

    def halo_start(*args):
        for n, (d_row, d_col) in enumerate(DIRS):
            @pl.when(inside(d_row, d_col))
            def _(n=n):
                halo_copy(*args, n).start()

    def halo_wait(*args):
        for n, (d_row, d_col) in enumerate(DIRS):
            @pl.when(inside(d_row, d_col))
            def _(n=n):
                halo_copy(*args, n).wait_send()

            @pl.when(inside(-d_row, -d_col))
            def _(n=n):
                halo_copy(*args, n).wait_recv()

    def halo_zero(mid, left, right):
        @pl.when(row == 0)
        def _():
            for i in range(IMGS):
                mid[i, 0] = jnp.zeros((COLS, CH), BF16)
                left[i, 0] = jnp.zeros((STRIP, CH), BF16)
                right[i, 0] = jnp.zeros((STRIP, CH), BF16)

        @pl.when(row == nrow - 1)
        def _():
            for i in range(IMGS):
                mid[i, ROWS + 1] = jnp.zeros((COLS, CH), BF16)
                left[i, ROWS + 1] = jnp.zeros((STRIP, CH), BF16)
                right[i, ROWS + 1] = jnp.zeros((STRIP, CH), BF16)

        for side, edge in ((left, 0), (right, ncol - 1)):
            @pl.when(col == edge)
            def _(side=side):
                @pl.loop(0, ROWS + 2)
                def _(r):
                    for i in range(IMGS):
                        side[i, r] = jnp.zeros((STRIP, CH), BF16)

    def store_sides(mid, side, i, r):
        for lane in range(0, CH, 128):
            val = mid[i, r, :, lane:lane + 128].astype(F32)
            side[i, r, :, lane:lane + 128] = pltpu.roll(val, COLS - 1, axis=0).astype(BF16)
            side[i, r, :, CH + lane:CH + lane + 128] = pltpu.roll(val, 1, axis=0).astype(BF16)

    def fix_edges(mid, side, left, right, i):
        for r in (0, ROWS + 1):
            store_sides(mid, side, i, r)
        at = lax.broadcasted_iota(jnp.int32, (STRIP, CH), 0)

        @pl.loop(0, ROWS + 2)
        def _(r):
            here = side[i, r, 0:STRIP, CH:2 * CH].astype(F32)
            other = pltpu.roll(left[i, r].astype(F32), 1, axis=0)
            side[i, r, 0:STRIP, CH:2 * CH] = jnp.where(at == 0, other, here).astype(BF16)
            here = side[i, r, COLS - STRIP:COLS, 0:CH].astype(F32)
            other = pltpu.roll(right[i, r].astype(F32), STRIP - 1, axis=0)
            side[i, r, COLS - STRIP:COLS, 0:CH] = jnp.where(at == STRIP - 1, other, here).astype(BF16)

    g_halo = (g_hbm, 0, gc, ghl, ghr, gs_sem, gr_sem)
    d_halo = (dc, 1, dc, dhl, dhr, ds_sem, dr_sem)
    for i in range(IMGS):
        halo_start(*g_halo, i)
    halo_zero(gc, ghl, ghr)
    halo_zero(dc, dhl, dhr)

    w_load2.wait()

    def slot_of(k):
        return k - lax.rem(k, 3) + lax.rem(2 * lax.rem(k, 3), 3)

    @pl.loop(0, 9)
    def _(k):
        w2t[slot_of(k)] = wraw[k].T

    w_load1.start()
    for load in x_loads:
        load.start()
    for i in range(IMGS):
        g_loads[i].wait()

        @pl.loop(0, ROWS)
        def _(r, i=i):
            store_sides(gc, gs, i, r + 1)

    def act_row(i, r):
        for j in range(0, COLS, PIX):
            z_val = gelu(abuf[i, r, j:j + PIX].astype(F32))
            zt[:, pl.ds(pl.multiple_of((i * ROWS + r) * COLS + j, PIX), PIX)] = z_val.astype(BF16).T

    for i in range(IMGS):
        a_loads[i].wait()

        @pl.loop(0, ROWS)
        def _(r, i=i):
            act_row(i, r)

    def place(blk):
        return lax.div(blk, ROWS // BLK), lax.rem(blk, ROWS // BLK) * BLK

    def conv(mid, side, weights, blk):
        i, r0 = place(blk)
        for half, out in ((0, s0), (1, s1)):
            total = None
            for a in range(3):
                rows = pl.ds(r0 + half * HALF + 2 - a, HALF)
                part = jnp.dot(side[i, rows].reshape(HALF * COLS, 2 * CH), weights[3 * a:3 * a + 2].reshape(2 * CH, CH),
                               preferred_element_type=F32)
                part = part + jnp.dot(mid[i, rows].reshape(HALF * COLS, CH), weights[3 * a + 2], preferred_element_type=F32)
                total = part if total is None else total + part
            out[...] = total

    def held_part(k, j, size=PIX):
        at = (k % HALF) * COLS + j
        return (s0 if k < HALF else s1)[at:at + size]

    def grad_rows(blk):
        i, r0 = place(blk)
        for k in range(BLK):
            for j in range(0, COLS, PIX):
                at = pl.multiple_of((i * ROWS + r0 + k) * COLS + j, PIX)
                xt[:, pl.ds(at, PIX)] = dc[i, r0 + k + 1, j:j + PIX].T
        for k in range(BLK):
            for lane in range(2):
                lanes = slice(128 * lane, 128 * lane + 128)
                at = (k % HALF) * COLS
                prod = (s0 if k < HALF else s1)[at:at + COLS, lanes] * gelu_slope(abuf[i, r0 + k, :, lanes].astype(F32))
                line = lines.at[2 * k + lane]
                line[8:8 + COLS] = prod
                dc[i, r0 + k + 1, :, lanes] = prod.astype(BF16)
                ds[i, r0 + k + 1, :, 128 * lane:128 * lane + 128] = line[9:9 + COLS].astype(BF16)
                ds[i, r0 + k + 1, :, CH + 128 * lane:CH + 128 * lane + 128] = line[7:7 + COLS].astype(BF16)

    def stages_of(p, c):
        return STAGES[c]

    def sizes(stages):
        out, rows, at = [], CH, 0
        for stage in stages:
            rows //= 2 ** len(stage)
            out.append((rows, at))
            at += (2 ** len(stage) - 1) * rows
        return out

    def start_at(stages, s):
        at = 0
        for stage, (h, _) in zip(stages[:s], sizes(stages)):
            at = at + seat(stage) * h
        return at

    def masks(stage):
        return range(1, 2 ** len(stage))

    def reduce_copy(p, c, s, m):
        idx, stages = p * 3 + c, stages_of(p, c)
        h, slot = sizes(stages)[s]
        src = acc.at[idx, pl.ds(pl.multiple_of(start_at(stages, s) + seat(stages[s], m) * h, 8), h)]
        return pltpu.make_async_remote_copy(src_ref=src, dst_ref=rbuf.at[idx, pl.ds(slot + (m - 1) * h, h)],
                                            send_sem=as_sem.at[idx, s + m - 1], recv_sem=ar_sem.at[idx, s + m - 1],
                                            device_id=partner(stages[s], m), device_id_type=MESH)

    def gather_copy(p, c, s, m):
        idx, stages = p * 3 + c, stages_of(p, c)
        part = res.at[idx, pl.ds(pl.multiple_of(start_at(stages, s + 1), 8), sizes(stages)[s][0])]
        k = MAXCOPY + s + m - 1
        return pltpu.make_async_remote_copy(src_ref=part, dst_ref=part, send_sem=as_sem.at[idx, k], recv_sem=ar_sem.at[idx, k],
                                            device_id=partner(stages[s], m), device_id_type=MESH)

    def out_copy(p, c):
        target = dw2_hbm if p < 3 else dw1_hbm
        idx = p * 3 + c
        return pltpu.make_async_copy(res.at[idx], target.at[idx % 9], out_sem.at[NBLK + idx])

    def reduce_start(p):
        for c in range(3):
            reduce_copy(p, c, 0, 1).start()

    def reduce_step(p, step):
        for c in range(3):
            idx, stages = p * 3 + c, stages_of(p, c)
            count = len(stages)
            if step < count:
                h, slot = sizes(stages)[step]
                keep = pl.ds(pl.multiple_of(start_at(stages, step + 1), 8), h)
                for m in masks(stages[step]):
                    reduce_copy(p, c, step, m).wait()
                total = acc[idx, keep]
                for m in masks(stages[step]):
                    total = total + rbuf[idx, slot + (m - 1) * h:slot + m * h]
                if step < count - 1:
                    acc[idx, keep] = total
                    for m in masks(stages[step + 1]):
                        reduce_copy(p, c, step + 1, m).start()
                else:
                    res[idx, keep] = total
                    for m in masks(stages[step]):
                        gather_copy(p, c, step, m).start()
            else:
                s = 2 * count - 1 - step
                for m in masks(stages[s]):
                    gather_copy(p, c, s, m).wait()
                if s > 0:
                    for m in masks(stages[s - 1]):
                        gather_copy(p, c, s - 1, m).start()
                else:
                    out_copy(p, c).start()

    grad_ticks = ((0, 0), (0, 1), (1, 0), (1, 1), (2, 0), (2, 1))
    late_ticks = ((3, 0), (4, 0), (3, 1), (4, 1), (5, 0), (5, 1))
    late_first = 3 * NCHUNK + NBLK - 1
    dx_first = late_first + len(late_ticks)
    last_tick = dx_first + NBLK - 1
    ready = {p: n + 1 for n, (p, _) in enumerate(grad_ticks)}
    ready.update({p: late_first + n + 1 for n, (p, _) in enumerate(late_ticks)})
    table = {}
    for p in range(6):
        for step, delay in enumerate(EARLY if p < 3 else LATE):
            table.setdefault(ready[p] + delay - 1, []).append((p, step))

    def run_steps(at):
        for p, step in table.get(at, ()):
            reduce_step(p, step)

    def tick(now, lo, hi):
        for at in sorted(table):
            if lo <= at < hi:
                @pl.when(now == at)
                def _(at=at):
                    run_steps(at)

    def weight_grad(p, n, lhs, mid, side):
        a = p % 3
        left = lhs[:, n * CHUNK * COLS:(n + 1) * CHUNK * COLS]
        part = jnp.dot(left, side[n, 2 - a:2 - a + CHUNK].reshape(CHUNK * COLS, 2 * CH), preferred_element_type=F32)
        for c, val in ((0, part[:, :CH]), (2, part[:, CH:])):
            acc[p * 3 + c] = val if n == 0 else acc[p * 3 + c] + val
        for top in range(0, CH, PIX):
            rows = slice(top, top + PIX)
            val = jnp.dot(left[rows], mid[n, 2 - a:2 - a + CHUNK].reshape(CHUNK * COLS, CH), preferred_element_type=F32)
            acc[p * 3 + 1, rows] = val if n == 0 else acc[p * 3 + 1, rows] + val

    def turn_weights(now):
        for k in range(2 * now, min(2 * now + 2, 9)):
            w1t[slot_of(k)] = wraw[k].T

    for i in range(IMGS):
        halo_wait(*g_halo, i)
        fix_edges(gc, gs, ghl, ghr, i)
    for now, (p, n) in enumerate(grad_ticks):
        weight_grad(p, n, zt, gc, gs)
        if n == 1:
            reduce_start(p)
        run_steps(now)

    for load in x_loads:
        load.wait()
    half_blocks = NBLK // IMGS
    dz_first = 3 * NCHUNK
    dz_last = dz_first + NBLK - 1
    conv(gc, gs, w2t, 0)

    def dz_step(n):
        grad_rows(n)
        conv(gc, gs, w2t, n + 1)
        tick(dz_first + n, dz_first, dz_last)

    @pl.loop(0, half_blocks)
    def _(n):
        dz_step(n)

    halo_start(*d_halo, 0)

    @pl.loop(half_blocks, NBLK - 1)
    def _(n):
        dz_step(n)

    grad_rows(NBLK - 1)
    halo_start(*d_halo, 1)
    halo_wait(*d_halo, 0)
    fix_edges(dc, ds, dhl, dhr, 0)
    w_load1.wait()

    for now, (p, n) in enumerate(late_ticks):
        if (p, n) == (3, 1):
            halo_wait(*d_halo, 1)
            fix_edges(dc, ds, dhl, dhr, 1)
        turn_weights(now)
        weight_grad(p, n, xt, dc, ds)
        if n == 1:
            reduce_start(p)
        run_steps(late_first + now)

    def dx_out(blk):
        i, r0 = place(blk)
        return pltpu.make_async_copy(abuf.at[i, pl.ds(r0, BLK)], dx_hbm.at[i, pl.ds(r0, BLK)], out_sem.at[blk])

    def dx_rows(blk):
        i, r0 = place(blk)
        for k in range(BLK):
            for j in range(0, COLS, PIX):
                g_val = gc[i, r0 + k + 1, j:j + PIX].astype(F32)
                abuf[i, r0 + k, j:j + PIX] = (held_part(k, j) + g_val).astype(BF16)

    conv(dc, ds, w1t, 0)

    @pl.loop(0, NBLK - 1)
    def _(n):
        dx_rows(n)
        conv(dc, ds, w1t, n + 1)
        dx_out(n).start()
        tick(dx_first + n, dx_first, last_tick)

    dx_rows(NBLK - 1)
    dx_out(NBLK - 1).start()
    for at in sorted(table):
        if at >= last_tick:
            run_steps(at)
    for blk in range(NBLK):
        dx_out(blk).wait()
    for p in range(6):
        for c in range(3):
            out_copy(p, c).wait()


def solution(mesh):
    def local_step(x_tile, a_tile, g_tile, w_one, w_two):
        wide = (IMGS, ROWS + 2, COLS, 2 * CH)
        tall = (IMGS, ROWS + 2, COLS, CH)
        side = (IMGS, ROWS + 2, STRIP, CH)
        any_spec = pl.BlockSpec(memory_space=pl.ANY)
        d_x, d_w1, d_w2 = pl.pallas_call(
            kernel,
            out_shape=(jax.ShapeDtypeStruct(x_tile.shape, BF16),
                       jax.ShapeDtypeStruct((9, CH, CH), F32), jax.ShapeDtypeStruct((9, CH, CH), F32)),
            in_specs=[any_spec] * 5,
            out_specs=(any_spec,) * 3,
            scratch_shapes=[
                pltpu.VMEM(tall, BF16), pltpu.VMEM(wide, BF16), pltpu.VMEM(tall, BF16), pltpu.VMEM(wide, BF16),
                pltpu.VMEM((IMGS, ROWS, COLS, CH), BF16),
                pltpu.VMEM((CH, IMGS * ROWS * COLS), BF16), pltpu.VMEM((CH, IMGS * ROWS * COLS), BF16),
                pltpu.VMEM((9, CH, CH), BF16), pltpu.VMEM((9, CH, CH), BF16), pltpu.VMEM((9, CH, CH), BF16),
                pltpu.VMEM((2 * BLK, COLS + 16, 128), F32),
                pltpu.VMEM((18, CH, CH), F32), pltpu.VMEM((18, CH, CH), F32), pltpu.VMEM((18, CH, CH), F32),
                pltpu.VMEM((HALF * COLS, CH), F32), pltpu.VMEM((HALF * COLS, CH), F32),
                pltpu.VMEM(side, BF16), pltpu.VMEM(side, BF16), pltpu.VMEM(side, BF16), pltpu.VMEM(side, BF16),
                pltpu.SemaphoreType.DMA((4,)), pltpu.SemaphoreType.DMA((2,)), pltpu.SemaphoreType.DMA((NBLK + 18,)),
                pltpu.SemaphoreType.DMA((2,)),
                pltpu.SemaphoreType.DMA((2, 8)), pltpu.SemaphoreType.DMA((2, 8)), pltpu.SemaphoreType.DMA((2, 8)), pltpu.SemaphoreType.DMA((2, 8)),
                pltpu.SemaphoreType.DMA((18, 2 * MAXCOPY)), pltpu.SemaphoreType.DMA((18, 2 * MAXCOPY)),
            ],
            compiler_params=pltpu.CompilerParams(collective_id=0, has_side_effects=True, vmem_limit_bytes=67043328),
            name="conv_block_backward",
        )(x_tile, a_tile, g_tile, w_one.reshape(9, CH, CH), w_two.reshape(9, CH, CH))
        return d_x, d_w1.reshape(3, 3, CH, CH), d_w2.reshape(3, 3, CH, CH)

    tile_spec = P(None, "row", "col", None)
    return jax.shard_map(local_step, mesh=mesh, in_specs=(tile_spec, tile_spec, tile_spec, P(), P()), out_specs=(tile_spec, P(), P()), check_vma=False)
```

```python
import functools

import jax
import jax.numpy as jnp
from jax import lax
from jax.experimental import pallas as pl
from jax.experimental.pallas import tpu as pltpu
from jax.sharding import PartitionSpec as P

MESH = pl.DeviceIdType.MESH
F32 = jnp.float32
BF16 = jnp.bfloat16

IMGS, ROWS, COLS, CH = 2, 16, 256, 256
STRIP = 8
BLK = 4
HALF = BLK // 2
NBLK = IMGS * ROWS // BLK
CHUNK = 16
NCHUNK = IMGS * ROWS // CHUNK
DIRS = ((1, 0), (-1, 0), (0, 1), (0, -1), (1, 1), (1, -1), (-1, 1), (-1, -1))
CORE, XBIT, YBIT, ZNEAR, ZFAR = ("row", 1), ("row", 2), ("row", 4), ("col", 1), ("col", 2)
STAGES = (((CORE,), (XBIT,), (YBIT,), (ZNEAR, ZFAR)),
          ((CORE,), (YBIT,), (XBIT,), (ZNEAR, ZFAR)),
          ((CORE,), (ZNEAR,), (ZFAR,), (XBIT, YBIT)))
PEERS = ((CORE,), (XBIT,), (YBIT,), (ZNEAR,), (ZFAR,), (XBIT, YBIT), (ZNEAR, ZFAR))
MAXCOPY = 6
PIX = 128

EARLY = (1, 3, 5, 6, 8, 9, 11, 12)
LATE = (1, 2, 3, 4, 5, 6, 7, 8)


def gelu_tanh(a_val):
    scale = 0.7978845608028654
    square = (0.044715 * a_val) * a_val
    return jnp.tanh(scale * (a_val + square * a_val)), square


def gelu(a_val):
    tanh_val, _ = gelu_tanh(a_val)
    half = 0.5 * a_val
    return half + half * tanh_val


def gelu_slope(a_val):
    scale = 0.7978845608028654
    tanh_val, square = gelu_tanh(a_val)
    return (0.5 + 0.5 * tanh_val) + ((0.5 * a_val) * (1.0 - tanh_val * tanh_val)) * (scale * (1.0 + 3.0 * square))


def kernel(x_hbm, a_hbm, g_hbm, w1_hbm, w2_hbm, abuf, dw1_ref, dw2_ref,
           gc, gs, dc, ds, zt, xt, w1t, w2t, wraw, lines, acc, rbuf, s0, s1, ghl, ghr, dhl, dhr,
           load_sem, x_sem, w_sem, gs_sem, gr_sem, ds_sem, dr_sem, as_sem, ar_sem):
    row = lax.axis_index("row")
    col = lax.axis_index("col")
    nrow, ncol = 8, 4

    def bit_of(axis, bit):
        where = row if axis == "row" else col
        return lax.rem(lax.div(where, bit), 2)

    def flips(stage, mask):
        return [key for n, key in enumerate(stage) if (mask >> (len(stage) - 1 - n)) & 1]

    def partner(stage, mask):
        where = {"row": row, "col": col}
        for axis, bit in flips(stage, mask):
            where[axis] = where[axis] + bit * (1 - 2 * bit_of(axis, bit))
        return where

    def seat(stage, mask=0):
        flipped = flips(stage, mask)
        at = 0
        for key in stage:
            at = 2 * at + (1 - bit_of(*key) if key in flipped else bit_of(*key))
        return at

    def inside(d_row, d_col):
        ok = None
        for where, step, count in ((row, d_row, nrow), (col, d_col, ncol)):
            if step:
                cond = where < count - 1 if step > 0 else where > 0
                ok = cond if ok is None else jnp.logical_and(ok, cond)
        return ok

    barrier = pltpu.get_barrier_semaphore()
    for d_row, d_col in DIRS:
        @pl.when(inside(d_row, d_col))
        def _(d_row=d_row, d_col=d_col):
            pl.semaphore_signal(barrier, inc=1, device_id={"row": row + d_row, "col": col + d_col}, device_id_type=MESH)
    for stage in PEERS:
        pl.semaphore_signal(barrier, inc=1, device_id=partner(stage, 2 ** len(stage) - 1), device_id_type=MESH)

    g_loads = [pltpu.make_async_copy(g_hbm.at[i], gc.at[i, pl.ds(1, ROWS)], load_sem.at[i]) for i in range(IMGS)]
    a_loads = [pltpu.make_async_copy(a_hbm.at[i], abuf.at[i], load_sem.at[IMGS + i]) for i in range(IMGS)]
    w_load2 = pltpu.make_async_copy(w2_hbm, wraw, w_sem.at[0])
    w_load1 = pltpu.make_async_copy(w1_hbm, wraw, w_sem.at[1])
    w_load2.start()
    for load in g_loads + a_loads:
        load.start()

    x_loads = [pltpu.make_async_copy(x_hbm.at[i], dc.at[i, pl.ds(1, ROWS)], x_sem.at[i]) for i in range(IMGS)]

    def near(where, count):
        return 3 - jnp.where(where == 0, 1, 0) - jnp.where(where == count - 1, 1, 0)

    pl.semaphore_wait(barrier, len(PEERS) + near(row, nrow) * near(col, ncol) - 1)

    def halo_copy(src, row0, mid, left, right, send_sem, recv_sem, i, n):
        d_row, d_col = DIRS[n]
        s_row = pl.ds(row0, ROWS) if d_row == 0 else (row0 + ROWS - 1 if d_row > 0 else row0)
        t_row = pl.ds(1, ROWS) if d_row == 0 else (0 if d_row > 0 else ROWS + 1)
        if d_col == 0:
            s_ref, t_ref = src.at[i, s_row], mid.at[i, t_row]
        else:
            s_col = pl.ds(COLS - STRIP, STRIP) if d_col > 0 else pl.ds(0, STRIP)
            s_ref, t_ref = src.at[i, s_row, s_col], (left if d_col > 0 else right).at[i, t_row]
        return pltpu.make_async_remote_copy(src_ref=s_ref, dst_ref=t_ref, send_sem=send_sem.at[i, n], recv_sem=recv_sem.at[i, n],
                                            device_id={"row": row + d_row, "col": col + d_col}, device_id_type=MESH)

    def halo_start(*args):
        for n, (d_row, d_col) in enumerate(DIRS):
            @pl.when(inside(d_row, d_col))
            def _(n=n):
                halo_copy(*args, n).start()

    def halo_wait(*args):
        for n, (d_row, d_col) in enumerate(DIRS):
            @pl.when(inside(d_row, d_col))
            def _(n=n):
                halo_copy(*args, n).wait_send()

            @pl.when(inside(-d_row, -d_col))
            def _(n=n):
                halo_copy(*args, n).wait_recv()

    def halo_zero(mid, left, right):
        @pl.when(row == 0)
        def _():
            for i in range(IMGS):
                mid[i, 0] = jnp.zeros((COLS, CH), BF16)
                left[i, 0] = jnp.zeros((STRIP, CH), BF16)
                right[i, 0] = jnp.zeros((STRIP, CH), BF16)

        @pl.when(row == nrow - 1)
        def _():
            for i in range(IMGS):
                mid[i, ROWS + 1] = jnp.zeros((COLS, CH), BF16)
                left[i, ROWS + 1] = jnp.zeros((STRIP, CH), BF16)
                right[i, ROWS + 1] = jnp.zeros((STRIP, CH), BF16)

        for side, edge in ((left, 0), (right, ncol - 1)):
            @pl.when(col == edge)
            def _(side=side):
                @pl.loop(0, ROWS + 2)
                def _(r):
                    for i in range(IMGS):
                        side[i, r] = jnp.zeros((STRIP, CH), BF16)

    def store_sides(mid, side, i, r):
        for lane in range(0, CH, 128):
            val = mid[i, r, :, lane:lane + 128].astype(F32)
            side[i, r, :, lane:lane + 128] = pltpu.roll(val, COLS - 1, axis=0).astype(BF16)
            side[i, r, :, CH + lane:CH + lane + 128] = pltpu.roll(val, 1, axis=0).astype(BF16)

    def fix_edges(mid, side, left, right, i):
        for r in (0, ROWS + 1):
            store_sides(mid, side, i, r)
        at = lax.broadcasted_iota(jnp.int32, (STRIP, CH), 0)

        @pl.loop(0, ROWS + 2)
        def _(r):
            here = side[i, r, 0:STRIP, CH:2 * CH].astype(F32)
            other = pltpu.roll(left[i, r].astype(F32), 1, axis=0)
            side[i, r, 0:STRIP, CH:2 * CH] = jnp.where(at == 0, other, here).astype(BF16)
            here = side[i, r, COLS - STRIP:COLS, 0:CH].astype(F32)
            other = pltpu.roll(right[i, r].astype(F32), STRIP - 1, axis=0)
            side[i, r, COLS - STRIP:COLS, 0:CH] = jnp.where(at == STRIP - 1, other, here).astype(BF16)

    g_halo = (g_hbm, 0, gc, ghl, ghr, gs_sem, gr_sem)
    d_halo = (dc, 1, dc, dhl, dhr, ds_sem, dr_sem)
    for i in range(IMGS):
        halo_start(*g_halo, i)
    halo_zero(gc, ghl, ghr)
    halo_zero(dc, dhl, dhr)

    w_load2.wait()

    def slot_of(k):
        return k - lax.rem(k, 3) + lax.rem(2 * lax.rem(k, 3), 3)

    @pl.loop(0, 9)
    def _(k):
        w2t[slot_of(k)] = wraw[k].T

    w_load1.start()
    for load in x_loads:
        load.start()
    for i in range(IMGS):
        g_loads[i].wait()

        @pl.loop(0, ROWS)
        def _(r, i=i):
            store_sides(gc, gs, i, r + 1)

    def act_row(i, r):
        for j in range(0, COLS, PIX):
            z_val = gelu(abuf[i, r, j:j + PIX].astype(F32))
            zt[:, pl.ds(pl.multiple_of((i * ROWS + r) * COLS + j, PIX), PIX)] = z_val.astype(BF16).T

    for i in range(IMGS):
        a_loads[i].wait()

        @pl.loop(0, ROWS)
        def _(r, i=i):
            act_row(i, r)

    def place(blk):
        return lax.div(blk, ROWS // BLK), lax.rem(blk, ROWS // BLK) * BLK

    def conv(mid, side, weights, blk):
        i, r0 = place(blk)
        for half, out in ((0, s0), (1, s1)):
            total = None
            for a in range(3):
                rows = pl.ds(r0 + half * HALF + 2 - a, HALF)
                part = jnp.dot(side[i, rows].reshape(HALF * COLS, 2 * CH), weights[3 * a:3 * a + 2].reshape(2 * CH, CH),
                               preferred_element_type=F32)
                part = part + jnp.dot(mid[i, rows].reshape(HALF * COLS, CH), weights[3 * a + 2], preferred_element_type=F32)
                total = part if total is None else total + part
            out[...] = total

    def held_part(k, j, size=PIX):
        at = (k % HALF) * COLS + j
        return (s0 if k < HALF else s1)[at:at + size]

    def grad_rows(blk):
        i, r0 = place(blk)
        for k in range(BLK):
            for j in range(0, COLS, PIX):
                at = pl.multiple_of((i * ROWS + r0 + k) * COLS + j, PIX)
                xt[:, pl.ds(at, PIX)] = dc[i, r0 + k + 1, j:j + PIX].T
        for k in range(BLK):
            for lane in range(2):
                lanes = slice(128 * lane, 128 * lane + 128)
                at = (k % HALF) * COLS
                prod = (s0 if k < HALF else s1)[at:at + COLS, lanes] * gelu_slope(abuf[i, r0 + k, :, lanes].astype(F32))
                line = lines.at[2 * k + lane]
                line[8:8 + COLS] = prod
                dc[i, r0 + k + 1, :, lanes] = prod.astype(BF16)
                ds[i, r0 + k + 1, :, 128 * lane:128 * lane + 128] = line[9:9 + COLS].astype(BF16)
                ds[i, r0 + k + 1, :, CH + 128 * lane:CH + 128 * lane + 128] = line[7:7 + COLS].astype(BF16)

    def stages_of(p, c):
        return STAGES[c]

    def sizes(stages):
        out, rows, at = [], CH, 0
        for stage in stages:
            rows //= 2 ** len(stage)
            out.append((rows, at))
            at += (2 ** len(stage) - 1) * rows
        return out

    def start_at(stages, s):
        at = 0
        for stage, (h, _) in zip(stages[:s], sizes(stages)):
            at = at + seat(stage) * h
        return at

    def masks(stage):
        return range(1, 2 ** len(stage))

    def reduce_copy(p, c, s, m):
        idx, stages = p * 3 + c, stages_of(p, c)
        h, slot = sizes(stages)[s]
        src = acc.at[idx, pl.ds(pl.multiple_of(start_at(stages, s) + seat(stages[s], m) * h, 8), h)]
        return pltpu.make_async_remote_copy(src_ref=src, dst_ref=rbuf.at[idx, pl.ds(slot + (m - 1) * h, h)],
                                            send_sem=as_sem.at[idx, s + m - 1], recv_sem=ar_sem.at[idx, s + m - 1],
                                            device_id=partner(stages[s], m), device_id_type=MESH)

    def gather_copy(p, c, s, m):
        idx, stages = p * 3 + c, stages_of(p, c)
        part = (dw2_ref if p < 3 else dw1_ref).at[idx % 9, pl.ds(pl.multiple_of(start_at(stages, s + 1), 8), sizes(stages)[s][0])]
        k = MAXCOPY + s + m - 1
        return pltpu.make_async_remote_copy(src_ref=part, dst_ref=part, send_sem=as_sem.at[idx, k], recv_sem=ar_sem.at[idx, k],
                                            device_id=partner(stages[s], m), device_id_type=MESH)

    def reduce_start(p):
        for c in range(3):
            reduce_copy(p, c, 0, 1).start()

    def reduce_step(p, step):
        for c in range(3):
            idx, stages = p * 3 + c, stages_of(p, c)
            count = len(stages)
            if step < count:
                h, slot = sizes(stages)[step]
                keep = pl.ds(pl.multiple_of(start_at(stages, step + 1), 8), h)
                for m in masks(stages[step]):
                    reduce_copy(p, c, step, m).wait()
                total = acc[idx, keep]
                for m in masks(stages[step]):
                    total = total + rbuf[idx, slot + (m - 1) * h:slot + m * h]
                if step < count - 1:
                    acc[idx, keep] = total
                    for m in masks(stages[step + 1]):
                        reduce_copy(p, c, step + 1, m).start()
                else:
                    (dw2_ref if p < 3 else dw1_ref)[idx % 9, keep] = total
                    for m in masks(stages[step]):
                        gather_copy(p, c, step, m).start()
            else:
                s = 2 * count - 1 - step
                for m in masks(stages[s]):
                    gather_copy(p, c, s, m).wait()
                if s > 0:
                    for m in masks(stages[s - 1]):
                        gather_copy(p, c, s - 1, m).start()

    grad_ticks = ((0, 0), (0, 1), (1, 0), (1, 1), (2, 0), (2, 1))
    late_ticks = ((3, 0), (4, 0), (3, 1), (4, 1), (5, 0), (5, 1))
    late_first = 3 * NCHUNK + NBLK - 1
    dx_first = late_first + len(late_ticks)
    last_tick = dx_first + NBLK - 1
    ready = {p: n + 1 for n, (p, _) in enumerate(grad_ticks)}
    ready.update({p: late_first + n + 1 for n, (p, _) in enumerate(late_ticks)})
    table = {}
    for p in range(6):
        for step, delay in enumerate(EARLY if p < 3 else LATE):
            table.setdefault(ready[p] + delay - 1, []).append((p, step))

    def run_steps(at):
        for p, step in table.get(at, ()):
            reduce_step(p, step)

    def tick(now, lo, hi):
        for at in sorted(table):
            if lo <= at < hi:
                @pl.when(now == at)
                def _(at=at):
                    run_steps(at)

    def weight_grad(p, n, lhs, mid, side):
        a = p % 3
        left = lhs[:, n * CHUNK * COLS:(n + 1) * CHUNK * COLS]
        part = jnp.dot(left, side[n, 2 - a:2 - a + CHUNK].reshape(CHUNK * COLS, 2 * CH), preferred_element_type=F32)
        for c, val in ((0, part[:, :CH]), (2, part[:, CH:])):
            acc[p * 3 + c] = val if n == 0 else acc[p * 3 + c] + val
        for top in range(0, CH, PIX):
            rows = slice(top, top + PIX)
            val = jnp.dot(left[rows], mid[n, 2 - a:2 - a + CHUNK].reshape(CHUNK * COLS, CH), preferred_element_type=F32)
            acc[p * 3 + 1, rows] = val if n == 0 else acc[p * 3 + 1, rows] + val

    def turn_weights(now):
        for k in range(2 * now, min(2 * now + 2, 9)):
            w1t[slot_of(k)] = wraw[k].T

    for i in range(IMGS):
        halo_wait(*g_halo, i)
        fix_edges(gc, gs, ghl, ghr, i)
    for now, (p, n) in enumerate(grad_ticks):
        weight_grad(p, n, zt, gc, gs)
        if n == 1:
            reduce_start(p)
        run_steps(now)

    for load in x_loads:
        load.wait()
    half_blocks = NBLK // IMGS
    dz_first = 3 * NCHUNK
    dz_last = dz_first + NBLK - 1
    conv(gc, gs, w2t, 0)

    def dz_step(n):
        grad_rows(n)
        conv(gc, gs, w2t, n + 1)
        tick(dz_first + n, dz_first, dz_last)

    @pl.loop(0, half_blocks)
    def _(n):
        dz_step(n)

    halo_start(*d_halo, 0)

    @pl.loop(half_blocks, NBLK - 1)
    def _(n):
        dz_step(n)

    grad_rows(NBLK - 1)
    halo_start(*d_halo, 1)
    halo_wait(*d_halo, 0)
    fix_edges(dc, ds, dhl, dhr, 0)
    w_load1.wait()

    for now, (p, n) in enumerate(late_ticks):
        if (p, n) == (3, 1):
            halo_wait(*d_halo, 1)
            fix_edges(dc, ds, dhl, dhr, 1)
        turn_weights(now)
        weight_grad(p, n, xt, dc, ds)
        if n == 1:
            reduce_start(p)
        run_steps(late_first + now)

    def dx_rows(blk):
        i, r0 = place(blk)
        for k in range(BLK):
            for j in range(0, COLS, PIX):
                g_val = gc[i, r0 + k + 1, j:j + PIX].astype(F32)
                abuf[i, r0 + k, j:j + PIX] = (held_part(k, j) + g_val).astype(BF16)

    conv(dc, ds, w1t, 0)

    @pl.loop(0, NBLK - 1)
    def _(n):
        dx_rows(n)
        conv(dc, ds, w1t, n + 1)
        tick(dx_first + n, dx_first, last_tick)

    dx_rows(NBLK - 1)
    for at in sorted(table):
        if at >= last_tick:
            run_steps(at)


def solution(mesh):
    def local_step(x_tile, a_tile, g_tile, w_one, w_two):
        wide = (IMGS, ROWS + 2, COLS, 2 * CH)
        tall = (IMGS, ROWS + 2, COLS, CH)
        side = (IMGS, ROWS + 2, STRIP, CH)
        any_spec = pl.BlockSpec(memory_space=pl.ANY)
        d_x, d_w1, d_w2 = pl.pallas_call(
            kernel,
            out_shape=(pltpu.VMEM(x_tile.shape, BF16), pltpu.VMEM((9, CH, CH), F32), pltpu.VMEM((9, CH, CH), F32)),
            in_specs=[any_spec] * 5,
            out_specs=(pl.BlockSpec(memory_space=pltpu.VMEM),) * 3,
            scratch_shapes=[
                pltpu.VMEM(tall, BF16), pltpu.VMEM(wide, BF16), pltpu.VMEM(tall, BF16), pltpu.VMEM(wide, BF16),
                pltpu.VMEM((CH, IMGS * ROWS * COLS), BF16), pltpu.VMEM((CH, IMGS * ROWS * COLS), BF16),
                pltpu.VMEM((9, CH, CH), BF16), pltpu.VMEM((9, CH, CH), BF16), pltpu.VMEM((9, CH, CH), BF16),
                pltpu.VMEM((2 * BLK, COLS + 16, 128), F32),
                pltpu.VMEM((18, CH, CH), F32), pltpu.VMEM((18, CH, CH), F32),
                pltpu.VMEM((HALF * COLS, CH), F32), pltpu.VMEM((HALF * COLS, CH), F32),
                pltpu.VMEM(side, BF16), pltpu.VMEM(side, BF16), pltpu.VMEM(side, BF16), pltpu.VMEM(side, BF16),
                pltpu.SemaphoreType.DMA((4,)), pltpu.SemaphoreType.DMA((2,)),
                pltpu.SemaphoreType.DMA((2,)),
                pltpu.SemaphoreType.DMA((2, 8)), pltpu.SemaphoreType.DMA((2, 8)), pltpu.SemaphoreType.DMA((2, 8)), pltpu.SemaphoreType.DMA((2, 8)),
                pltpu.SemaphoreType.DMA((18, 2 * MAXCOPY)), pltpu.SemaphoreType.DMA((18, 2 * MAXCOPY)),
            ],
            compiler_params=pltpu.CompilerParams(collective_id=0, has_side_effects=True, vmem_limit_bytes=57000000),
            name="conv_block_backward",
        )(x_tile, a_tile, g_tile, w_one.reshape(9, CH, CH), w_two.reshape(9, CH, CH))
        return d_x, d_w1.reshape(3, 3, CH, CH), d_w2.reshape(3, 3, CH, CH)

    tile_spec = P(None, "row", "col", None)
    return jax.shard_map(local_step, mesh=mesh, in_specs=(tile_spec, tile_spec, tile_spec, P(), P()), out_specs=(tile_spec, P(), P()), check_vma=False)
```
